32 devices in a mesh: tm: 2 (over x), member: 4 (over y, core), state: 4 (over z).
Axes of the slice: x: 2, y: 2, z: 4, core: 2. Of those that a mesh axis runs over, the one named last changes fastest.
Arguments:
- members: bfloat16 [4, 8, 16, 192, 1536], P('tm', 'member', None, 'state'), may hold values from -6 to 6
- slot_grad: float32 [4, 16, 192, 1536], P('tm', None, 'state'), may hold values from -6 to 6
- diffusivity: float32 [192, 1536], P('state'), may hold values from 0.03 to 0.24
- vertical: float32 [16, 16], replicated, may hold values from -0.3 to 2.1, as said below
Outputs:
- control_gradient: float32 [16, 8, 192, 1536], P('tm', 'member', 'state')
The draws below stay inside these ranges and needn't reach their ends.
Inputs may be any that keep to these rules, and one draw needn't show every extreme that they name: `vertical`: the diagonal entries lie between 0.5 and 2.1.
All inputs are finite; a program needn't handle non-finite values.
Results may differ from the reference program's by a relative error of at most 0.0003.
Values sent between devices are 32-bit elements; how exact they have to be, the bound alone decides.
No kernel may reach another device: no remote copies, remote signals or barrier semaphores. Data moves between devices by JAX's collectives and lax.ppermute only.
A program may use at most 128 MiB of HBM per device.

```python
import math
import jax
import jax.numpy as jnp
from jax import lax

LON = 1536
LEVELS = 16
NSTEP = 4
LAT = 192
MEMBERS = 8
SLOTS = 4


def draw_vertical(key, part):
    first_key, second_key = jax.random.split(jax.random.fold_in(key, 17))
    offdiag = jnp.clip(jax.random.normal(first_key, (LEVELS, LEVELS), jnp.float32), -3.0, 3.0) / 3.0
    diagonal = jnp.exp(jax.random.uniform(second_key, (LEVELS,), jnp.float32, -0.69, 0.69))
    identity = jnp.eye(LEVELS, dtype=jnp.float32)
    return 0.27 * offdiag * (1.0 - identity) + identity * diagonal[None, :]


def levels(stream_key, shape, pieces, smallest, top_value):
    level, own = 1.0, jax.random.fold_in(stream_key, 6)
    for axis_at, parts in pieces:
        heights = jnp.exp(jax.random.uniform(jax.random.fold_in(own, axis_at), (parts,), jnp.float32, smallest / len(pieces), top_value / len(pieces)))
        level = level * jnp.repeat(heights, shape[axis_at] // parts).reshape([-1 if axis == axis_at else 1 for axis in range(len(shape))])
    return level


def noise(stream_key, shape, width, limit, cuts=(), kind=jnp.bfloat16):
    gain = levels(stream_key, shape, cuts, -0.22, 0.18) if cuts else 1.0
    result = jax.random.normal(stream_key, shape, jnp.float32) * width * gain
    return jnp.minimum(jnp.maximum(result, -limit), limit).astype(kind)


def setup_inputs(seed: int = 0) -> dict:
    key_of = jax.random.split(jax.random.key(seed), 5)
    members = noise(key_of[0], (SLOTS, MEMBERS, LEVELS, LAT, LON), 1.0, 6.0, ((0, 2), (1, 4), (3, 4)))
    slot_grad = noise(key_of[1], (SLOTS, LEVELS, LAT, LON), 1.0, 6.0, ((0, 2), (2, 4)), jnp.float32)
    diffusivity = jnp.clip(jnp.exp(math.log(0.24) - 2.0794415 * jax.random.uniform(key_of[2], (LAT, LON), jnp.float32) ** levels(key_of[2], (LAT, LON), ((0, 4),), -0.2, 0.2)), 0.03, 0.24)
    vertical = draw_vertical(jax.random.fold_in(key_of[4], 71), 0)
    return dict(members=members, slot_grad=slot_grad, diffusivity=diffusivity, vertical=vertical)


def stencil_update(centre, spread):
    middle = spread[..., 1:-1, :]
    return centre + spread[..., 2:, :] + spread[..., :-2, :] + jnp.roll(middle, 1, -1) + jnp.roll(middle, -1, -1) - 4.0 * middle


def reference(members, slot_grad, diffusivity, vertical):
    ensemble = members.shape[1]
    spread_scale = float(ensemble - 1) ** -0.5
    centre = jnp.sum(members, axis=1, dtype=jnp.float32) / ensemble

    def member_product(which):
        single = lax.dynamic_index_in_dim(members, which, 1, keepdims=False).astype(jnp.float32)
        perturbed = (single - centre) * spread_scale
        return jnp.sum(perturbed * slot_grad, axis=0)

    partial_value = lax.map(member_product, jnp.arange(ensemble, dtype=jnp.int32))
    field = jnp.einsum("ml,kmab->lkab", vertical, partial_value, precision=lax.Precision.HIGHEST)
    for step_index in range(NSTEP):
        spread = jnp.pad(diffusivity * field, ((0, 0), (0, 0), (1, 1), (0, 0)))
        field = stencil_update(field, spread)
    return field
```

```python
import functools

import jax
import jax.numpy as jnp
from jax import lax
from jax.experimental import pallas as pl
from jax.experimental.pallas import tpu as pltpu
from jax.sharding import PartitionSpec as P


NSTEP = 4
SUB = 8


def level_chunks(count):
    sizes, left = [], count
    while left > 0:
        size = max(left // 2, 1)
        sizes.append(size)
        left -= size
    starts = [sum(sizes[:i]) for i in range(len(sizes))]
    return list(zip(starts, sizes))


def divisor(length, unit, most):
    best = unit
    for size in range(unit, most + 1, unit):
        if length % size == 0:
            best = size
    return best


def mix_kernel(chunks, lanes, w_ref, members_ref, grad_ref, *out_refs):
    slots, ensemble, levels, rows, cols = members_ref.shape
    w = w_ref[...]
    high = w.astype(jnp.bfloat16)
    low = (w - high.astype(jnp.float32)).astype(jnp.bfloat16)
    twice = jnp.concatenate([high, high], axis=1)

    def piece(index, carry):
        at = pl.ds(pl.multiple_of(index * lanes, lanes), lanes)
        grads = [grad_ref[s, :, :, at] for s in range(slots)]
        for k in range(ensemble):
            product = members_ref[0, k, :, :, at].astype(jnp.float32) * grads[0]
            for s in range(1, slots):
                product += members_ref[s, k, :, :, at].astype(jnp.float32) * grads[s]
            for first in range(0, rows, SUB):
                x = product[:, first : first + SUB].reshape(levels * SUB, lanes)
                x_high = x.astype(jnp.bfloat16)
                x_low = (x - x_high.astype(jnp.float32)).astype(jnp.bfloat16)
                y = jnp.dot(
                    twice,
                    jnp.concatenate([x_high, x_low], axis=0),
                    preferred_element_type=jnp.float32,
                ) + jnp.dot(low, x_high, preferred_element_type=jnp.float32)
                y = y.reshape(-1, SUB, lanes)
                for out_ref, (start, size) in zip(out_refs, chunks):
                    out_ref[:, k, first : first + SUB, at] = y[start : start + size]
        return carry

    lax.fori_loop(0, cols // lanes, piece, 0)


def mixed_levels(members, slot_grad, weights, chunks):
    slots, ensemble, levels, rows, cols = members.shape
    row_block, col_block = divisor(rows, SUB, 16), divisor(cols, 128, 512)
    lanes = divisor(col_block, 128, 256)
    shapes = [(size, ensemble, rows, cols) for _, size in chunks]
    own = weights.shape[0] // SUB
    return pl.pallas_call(
        functools.partial(mix_kernel, chunks, lanes),
        grid=(rows // row_block, cols // col_block),
        in_specs=[
            pl.BlockSpec(weights.shape, lambda i, j: (0, 0)),
            pl.BlockSpec(
                (slots, ensemble, levels, row_block, col_block), lambda i, j: (0, 0, 0, i, j)
            ),
            pl.BlockSpec((slots, levels, row_block, col_block), lambda i, j: (0, 0, i, j)),
        ],
        out_specs=[
            pl.BlockSpec((size, ensemble, row_block, col_block), lambda i, j: (0, 0, i, j))
            for _, size in chunks
        ],
        out_shape=[jax.ShapeDtypeStruct(shape, jnp.float32) for shape in shapes],
        cost_estimate=pl.CostEstimate(
            flops=6 * SUB * levels * own * ensemble * rows * cols,
            bytes_accessed=2 * members.size + 4 * slot_grad.size,
            transcendentals=0,
        ),
        name="mix",
    )(weights, members, slot_grad)


def filter_kernel(parts, halo, share, *refs):
    field_refs = refs[:parts]
    sum_ref, other_ref, above_ref, below_ref, rate_ref = refs[parts : parts + 5]
    out_ref, f_ref, v_ref = refs[-3:]
    rows, cols = out_ref.shape[2:]
    bands = rows // SUB + 2
    blank = jnp.zeros((SUB, cols), jnp.float32)
    for edge in (0, bands + 1):
        v_ref[edge * SUB : (edge + 1) * SUB] = blank
    for edge in (0, bands - 1):
        f_ref[edge * SUB : (edge + 1) * SUB] = blank
    f_ref[SUB - halo : SUB] = above_ref[0, 0]
    f_ref[SUB + rows : SUB + rows + halo] = below_ref[0, 0]
    for band in range(rows // SUB):
        at = slice(band * SUB, (band + 1) * SUB)
        value = field_refs[0][0, 0, at]
        for ref in field_refs[1:]:
            value += ref[0, 0, at]
        f_ref[SUB + band * SUB : SUB + (band + 1) * SUB] = value - share * (
            sum_ref[0, at] + other_ref[0, at]
        )
    for step in range(NSTEP):
        for band in range(bands):
            at = slice(band * SUB, (band + 1) * SUB)
            v_ref[SUB + band * SUB : 2 * SUB + band * SUB] = rate_ref[at] * f_ref[at]
        last = step == NSTEP - 1
        for band in range(1, bands - 1) if last else range(bands):
            at = slice(band * SUB, (band + 1) * SUB)
            base = SUB + band * SUB
            v = v_ref[base : base + SUB]
            value = (
                f_ref[at]
                + v_ref[base + 1 : base + 1 + SUB]
                + v_ref[base - 1 : base - 1 + SUB]
                + pltpu.roll(v, 1, 1)
                + pltpu.roll(v, cols - 1, 1)
                - 4.0 * v
            )
            if last:
                out_ref[0, 0, (band - 1) * SUB : band * SUB] = value
            else:
                f_ref[at] = value


def filtered(fields, sums, halos, rate, start, total, ensemble, previous):
    size, members, rows, cols = fields[0].shape
    halo = halos[0].shape[2]
    plane = pl.BlockSpec((1, 1, rows, cols), lambda i, k: (i, k, 0, 0))
    shared = pl.BlockSpec((1, rows, cols), lambda i, k: (i, 0, 0))
    edge = pl.BlockSpec((1, 1, halo, cols), lambda i, k: (i, k, 0, 0))
    operands = [*fields, *sums, *halos, rate]
    in_specs = [plane] * len(fields) + [shared] * 2 + [edge] * 2
    in_specs.append(pl.BlockSpec(rate.shape, lambda i, k: (0, 0)))
    aliases = {}
    if previous is not None:
        aliases = {len(operands): 0}
        operands.append(previous)
        in_specs.append(pl.BlockSpec(memory_space=pl.ANY))
    return pl.pallas_call(
        functools.partial(filter_kernel, len(fields), halo, 1.0 / ensemble),
        grid=(size, members),
        in_specs=in_specs,
        out_specs=pl.BlockSpec((1, 1, rows, cols), lambda i, k: (i + start, k, 0, 0)),
        out_shape=jax.ShapeDtypeStruct((total, members, rows, cols), jnp.float32),
        scratch_shapes=[
            pltpu.VMEM((rows + 2 * SUB, cols), jnp.float32),
            pltpu.VMEM((rows + 4 * SUB, cols), jnp.float32),
        ],
        input_output_aliases=aliases,
        cost_estimate=pl.CostEstimate(
            flops=40 * NSTEP * size * members * rows * cols,
            bytes_accessed=16 * size * members * rows * cols,
            transcendentals=0,
        ),
        name="filter",
    )(*operands)


def edges_from_neighbours(top, bottom):
    size = lax.axis_size("state")
    up = [(i, i + 1) for i in range(size - 1)]
    down = [(j, i) for i, j in up]
    return lax.ppermute(bottom, "state", up), lax.ppermute(top, "state", down)


def halves_of_sum(value):
    size = lax.axis_size("member")
    reach = 1
    other = jnp.zeros_like(value)
    if size & (size - 1):
        value, other = lax.psum(value, "member"), other
        return value, other
    while reach < size:
        pairs = [(i, i ^ reach) for i in range(size)]
        value = value + other if reach > 1 else value
        other = lax.ppermute(value, "member", pairs)
        reach *= 2
    return value, other


def compute(members, slot_grad, diffusivity, vertical):
    ensemble = members.shape[1] * lax.axis_size("member")
    levels, rows = members.shape[2:4]
    groups = lax.axis_size("tm")
    own = levels // groups
    here = lax.axis_index("tm")
    chunks = level_chunks(own)
    halo = NSTEP
    scaled = vertical.T * float(ensemble - 1) ** (-0.5)
    eye = jnp.eye(SUB, dtype=jnp.float32)

    def weights(shift):
        first = lax.rem(here + shift, groups) * own
        chosen = lax.dynamic_slice_in_dim(scaled, first, own, 0)
        return (chosen[:, None, :, None] * eye[None, :, None, :]).reshape(own * SUB, levels * SUB)

    arrived = []
    for shift in range(1, groups):
        outgoing = mixed_levels(members, slot_grad, weights(shift), chunks)
        pairs = [(i, (i + shift) % groups) for i in range(groups)]
        parts = []
        for part in outgoing:
            parts.append(lax.ppermute(part, "tm", pairs))
        arrived.append(parts)
    mine = mixed_levels(members, slot_grad, weights(0), chunks)

    above, below = edges_from_neighbours(diffusivity[:halo], diffusivity[rows - halo :])
    blank = jnp.zeros((SUB - halo, diffusivity.shape[1]), jnp.float32)
    rate = jnp.concatenate([blank, above, diffusivity, below, blank], axis=0)

    staged, before = [], None
    for index in range(len(chunks)):
        received = [parts[index] for parts in arrived]
        if before is not None:
            received, before = lax.optimization_barrier((received, before))
        fields = [mine[index]] + received
        local = functools.reduce(jnp.add, [f[:, k] for f in fields for k in range(f.shape[1])])
        before, other = halves_of_sum(local)
        staged.append([fields, before, other])

    result = None
    for index, (start, size) in enumerate(chunks):
        fields, *sums = staged[index]
        if index + 1 < len(chunks):
            sums, _ = lax.optimization_barrier((sums, staged[index + 1][1]))

        def edge(at):
            value = functools.reduce(jnp.add, [f[:, :, at] for f in fields])
            return value - (sums[0][:, at] + sums[1][:, at])[:, None] * (1.0 / ensemble)

        halos = edges_from_neighbours(edge(slice(0, halo)), edge(slice(rows - halo, rows)))
        result = filtered(fields, sums, halos, rate, start, own, ensemble, result)
    return result


def solution(mesh):
    in_specs = (
        P("tm", "member", None, "state", None),
        P("tm", None, "state", None),
        P("state", None),
        P(),
    )
    out_specs = P("tm", "member", "state", None)
    return jax.shard_map(compute, mesh=mesh, in_specs=in_specs, out_specs=out_specs, check_vma=False)
```

```python
import functools

import jax
import jax.numpy as jnp
from jax import lax
from jax.experimental import pallas as pl
from jax.experimental.pallas import tpu as pltpu
from jax.sharding import PartitionSpec as P


NSTEP = 4
SUB = 8


def level_chunks(count):
    first = count - count // 2
    return [(0, first), (first, count - first)] if count > first else [(0, first)]


def divisor(length, unit, most):
    best = unit
    for size in range(unit, most + 1, unit):
        if length % size == 0:
            best = size
    return best


def mix_kernel(chunks, lanes, w_ref, members_ref, grad_ref, *out_refs):
    slots, ensemble, levels, rows, cols = members_ref.shape
    w = w_ref[...]
    high = w.astype(jnp.bfloat16)
    low = (w - high.astype(jnp.float32)).astype(jnp.bfloat16)
    twice = jnp.concatenate([high, high], axis=1)

    def piece(index, carry):
        at = pl.ds(pl.multiple_of(index * lanes, lanes), lanes)
        grads = [grad_ref[s, :, :, at] for s in range(slots)]
        for k in range(ensemble):
            product = members_ref[0, k, :, :, at].astype(jnp.float32) * grads[0]
            for s in range(1, slots):
                product += members_ref[s, k, :, :, at].astype(jnp.float32) * grads[s]
            for first in range(0, rows, SUB):
                x = product[:, first : first + SUB].reshape(levels * SUB, lanes)
                x_high = x.astype(jnp.bfloat16)
                x_low = (x - x_high.astype(jnp.float32)).astype(jnp.bfloat16)
                y = jnp.dot(
                    twice,
                    jnp.concatenate([x_high, x_low], axis=0),
                    preferred_element_type=jnp.float32,
                ) + jnp.dot(low, x_high, preferred_element_type=jnp.float32)
                y = y.reshape(-1, SUB, lanes)
                for out_ref, (start, size) in zip(out_refs, chunks):
                    out_ref[:, k, first : first + SUB, at] = y[start : start + size]
        return carry

    lax.fori_loop(0, cols // lanes, piece, 0)


def mixed_levels(members, slot_grad, weights, chunks):
    slots, ensemble, levels, rows, cols = members.shape
    row_block, col_block = divisor(rows, SUB, 16), divisor(cols, 128, 512)
    lanes = divisor(col_block, 128, 256)
    shapes = [(size, ensemble, rows, cols) for _, size in chunks]
    own = weights.shape[0] // SUB
    return pl.pallas_call(
        functools.partial(mix_kernel, chunks, lanes),
        grid=(rows // row_block, cols // col_block),
        in_specs=[
            pl.BlockSpec(weights.shape, lambda i, j: (0, 0)),
            pl.BlockSpec(
                (slots, ensemble, levels, row_block, col_block), lambda i, j: (0, 0, 0, i, j)
            ),
            pl.BlockSpec((slots, levels, row_block, col_block), lambda i, j: (0, 0, i, j)),
        ],
        out_specs=[
            pl.BlockSpec((size, ensemble, row_block, col_block), lambda i, j: (0, 0, i, j))
            for _, size in chunks
        ],
        out_shape=[jax.ShapeDtypeStruct(shape, jnp.float32) for shape in shapes],
        cost_estimate=pl.CostEstimate(
            flops=6 * SUB * levels * own * ensemble * rows * cols,
            bytes_accessed=2 * members.size + 4 * slot_grad.size,
            transcendentals=0,
        ),
        name="mix",
    )(weights, members, slot_grad)


def filter_kernel(parts, halo, share, *refs):
    field_refs = refs[:parts]
    sum_ref, other_ref, above_ref, below_ref, rate_ref = refs[parts : parts + 5]
    out_ref, f_ref, v_ref = refs[-3:]
    rows, cols = out_ref.shape[2:]
    bands = rows // SUB + 2
    blank = jnp.zeros((SUB, cols), jnp.float32)
    for edge in (0, bands + 1):
        v_ref[edge * SUB : (edge + 1) * SUB] = blank
    for edge in (0, bands - 1):
        f_ref[edge * SUB : (edge + 1) * SUB] = blank
    f_ref[SUB - halo : SUB] = above_ref[0, 0]
    f_ref[SUB + rows : SUB + rows + halo] = below_ref[0, 0]
    for band in range(rows // SUB):
        at = slice(band * SUB, (band + 1) * SUB)
        value = field_refs[0][0, 0, at]
        for ref in field_refs[1:]:
            value += ref[0, 0, at]
        f_ref[SUB + band * SUB : SUB + (band + 1) * SUB] = value - share * (
            sum_ref[0, at] + other_ref[0, at]
        )
    for step in range(NSTEP):
        for band in range(bands):
            at = slice(band * SUB, (band + 1) * SUB)
            v_ref[SUB + band * SUB : 2 * SUB + band * SUB] = rate_ref[at] * f_ref[at]
        last = step == NSTEP - 1
        for band in range(1, bands - 1) if last else range(bands):
            at = slice(band * SUB, (band + 1) * SUB)
            base = SUB + band * SUB
            v = v_ref[base : base + SUB]
            value = (
                f_ref[at]
                + v_ref[base + 1 : base + 1 + SUB]
                + v_ref[base - 1 : base - 1 + SUB]
                + pltpu.roll(v, 1, 1)
                + pltpu.roll(v, cols - 1, 1)
                - 4.0 * v
            )
            if last:
                out_ref[0, 0, (band - 1) * SUB : band * SUB] = value
            else:
                f_ref[at] = value


def filtered(fields, sums, halos, rate, start, total, ensemble, previous):
    size, members, rows, cols = fields[0].shape
    halo = halos[0].shape[2]
    plane = pl.BlockSpec((1, 1, rows, cols), lambda i, k: (i, k, 0, 0))
    shared = pl.BlockSpec((1, rows, cols), lambda i, k: (i, 0, 0))
    edge = pl.BlockSpec((1, 1, halo, cols), lambda i, k: (i, k, 0, 0))
    operands = [*fields, *sums, *halos, rate]
    in_specs = [plane] * len(fields) + [shared] * 2 + [edge] * 2
    in_specs.append(pl.BlockSpec(rate.shape, lambda i, k: (0, 0)))
    aliases = {}
    if previous is not None:
        aliases = {len(operands): 0}
        operands.append(previous)
        in_specs.append(pl.BlockSpec(memory_space=pl.ANY))
    return pl.pallas_call(
        functools.partial(filter_kernel, len(fields), halo, 1.0 / ensemble),
        grid=(size, members),
        in_specs=in_specs,
        out_specs=pl.BlockSpec((1, 1, rows, cols), lambda i, k: (i + start, k, 0, 0)),
        out_shape=jax.ShapeDtypeStruct((total, members, rows, cols), jnp.float32),
        scratch_shapes=[
            pltpu.VMEM((rows + 2 * SUB, cols), jnp.float32),
            pltpu.VMEM((rows + 4 * SUB, cols), jnp.float32),
        ],
        input_output_aliases=aliases,
        cost_estimate=pl.CostEstimate(
            flops=40 * NSTEP * size * members * rows * cols,
            bytes_accessed=16 * size * members * rows * cols,
            transcendentals=0,
        ),
        name="filter",
    )(*operands)


def edges_from_neighbours(top, bottom):
    size = lax.axis_size("state")
    up = [(i, i + 1) for i in range(size - 1)]
    down = [(j, i) for i, j in up]
    return lax.ppermute(bottom, "state", up), lax.ppermute(top, "state", down)


def halves_of_sum(value):
    size = lax.axis_size("member")
    reach = 1
    other = jnp.zeros_like(value)
    if size & (size - 1):
        value, other = lax.psum(value, "member"), other
        return value, other
    while reach < size:
        pairs = [(i, i ^ reach) for i in range(size)]
        value = value + other if reach > 1 else value
        other = lax.ppermute(value, "member", pairs)
        reach *= 2
    return value, other


def compute(members, slot_grad, diffusivity, vertical):
    ensemble = members.shape[1] * lax.axis_size("member")
    levels, rows = members.shape[2:4]
    groups = lax.axis_size("tm")
    own = levels // groups
    here = lax.axis_index("tm")
    chunks = level_chunks(own)
    halo = NSTEP
    scaled = vertical.T * float(ensemble - 1) ** (-0.5)
    eye = jnp.eye(SUB, dtype=jnp.float32)

    def weights(shift):
        first = lax.rem(here + shift, groups) * own
        chosen = lax.dynamic_slice_in_dim(scaled, first, own, 0)
        return (chosen[:, None, :, None] * eye[None, :, None, :]).reshape(own * SUB, levels * SUB)

    share = 1.0 / ensemble

    def member_sums(fields):
        local = functools.reduce(jnp.add, [f[:, k] for f in fields for k in range(f.shape[1])])
        return halves_of_sum(local)

    arrived = []
    for shift in range(1, groups):
        outgoing = mixed_levels(members, slot_grad, weights(shift), chunks)
        pairs = [(i, (i + shift) % groups) for i in range(groups)]
        parts = []
        for index, part in enumerate(outgoing):
            if index:
                total = member_sums([part])
                part = part - ((total[0] + total[1]) * share)[:, None]
            parts.append(lax.ppermute(part, "tm", pairs))
        arrived.append(parts)
    mine = mixed_levels(members, slot_grad, weights(0), chunks)

    above, below = edges_from_neighbours(diffusivity[:halo], diffusivity[rows - halo :])
    blank = jnp.zeros((SUB - halo, diffusivity.shape[1]), jnp.float32)
    rate = jnp.concatenate([blank, above, diffusivity, below, blank], axis=0)

    early = [member_sums([part]) for part in mine[1:]]
    first = [mine[0]] + [parts[0] for parts in arrived]
    centres = [member_sums(first), *early]

    result = None
    for index, (start, size) in enumerate(chunks):
        fields = [mine[index]] + [parts[index] for parts in arrived]
        sums = centres[index]

        def edge(at):
            value = functools.reduce(jnp.add, [f[:, :, at] for f in fields])
            return value - (sums[0][:, at] + sums[1][:, at])[:, None] * share

        halos = edges_from_neighbours(edge(slice(0, halo)), edge(slice(rows - halo, rows)))
        result = filtered(fields, sums, halos, rate, start, own, ensemble, result)
    return result


def solution(mesh):
    in_specs = (
        P("tm", "member", None, "state", None),
        P("tm", None, "state", None),
        P("state", None),
        P(),
    )
    out_specs = P("tm", "member", "state", None)
    return jax.shard_map(compute, mesh=mesh, in_specs=in_specs, out_specs=out_specs, check_vma=False)
```

```python
import functools

import jax
import jax.numpy as jnp
from jax import lax
from jax.experimental import pallas as pl
from jax.experimental.pallas import tpu as pltpu
from jax.sharding import PartitionSpec as P


NSTEP = 4
SUB = 8


def level_chunks(count):
    first = count - count // 2
    return [(0, first), (first, count - first)] if count > first else [(0, first)]


def divisor(length, unit, most):
    best = unit
    for size in range(unit, most + 1, unit):
        if length % size == 0:
            best = size
    return best


def mix_kernel(chunks, lanes, w_ref, members_ref, grad_ref, *out_refs):
    slots, ensemble, levels, rows, cols = members_ref.shape
    w = w_ref[...]
    high = w.astype(jnp.bfloat16)
    low = (w - high.astype(jnp.float32)).astype(jnp.bfloat16)
    twice = jnp.concatenate([high, high], axis=1)

    def piece(index, carry):
        at = pl.ds(pl.multiple_of(index * lanes, lanes), lanes)
        grads = [grad_ref[s, :, :, at] for s in range(slots)]
        for k in range(ensemble):
            product = members_ref[0, k, :, :, at].astype(jnp.float32) * grads[0]
            for s in range(1, slots):
                product += members_ref[s, k, :, :, at].astype(jnp.float32) * grads[s]
            for first in range(0, rows, SUB):
                x = product[:, first : first + SUB].reshape(levels * SUB, lanes)
                x_high = x.astype(jnp.bfloat16)
                x_low = (x - x_high.astype(jnp.float32)).astype(jnp.bfloat16)
                y = jnp.dot(
                    twice,
                    jnp.concatenate([x_high, x_low], axis=0),
                    preferred_element_type=jnp.float32,
                ) + jnp.dot(low, x_high, preferred_element_type=jnp.float32)
                y = y.reshape(-1, SUB, lanes)
                for out_ref, (start, size) in zip(out_refs, chunks):
                    out_ref[k, :, first : first + SUB, at] = y[start : start + size]
        return carry

    lax.fori_loop(0, cols // lanes, piece, 0)


def mixed_levels(members, slot_grad, weights, chunks):
    slots, ensemble, levels, rows, cols = members.shape
    row_block, col_block = divisor(rows, SUB, 16), divisor(cols, 128, 512)
    lanes = divisor(col_block, 128, 256)
    shapes = [(ensemble, size, rows, cols) for _, size in chunks]
    own = weights.shape[0] // SUB
    return pl.pallas_call(
        functools.partial(mix_kernel, chunks, lanes),
        grid=(rows // row_block, cols // col_block),
        in_specs=[
            pl.BlockSpec(weights.shape, lambda i, j: (0, 0)),
            pl.BlockSpec(
                (slots, ensemble, levels, row_block, col_block), lambda i, j: (0, 0, 0, i, j)
            ),
            pl.BlockSpec((slots, levels, row_block, col_block), lambda i, j: (0, 0, i, j)),
        ],
        out_specs=[
            pl.BlockSpec((ensemble, size, row_block, col_block), lambda i, j: (0, 0, i, j))
            for _, size in chunks
        ],
        out_shape=[jax.ShapeDtypeStruct(shape, jnp.float32) for shape in shapes],
        cost_estimate=pl.CostEstimate(
            flops=6 * SUB * levels * own * ensemble * rows * cols,
            bytes_accessed=2 * members.size + 4 * slot_grad.size,
            transcendentals=0,
        ),
        name="mix",
    )(weights, members, slot_grad)


def filter_kernel(parts, halo, share, *refs):
    field_refs = refs[:parts]
    sum_ref, other_ref, above_ref, below_ref, rate_ref = refs[parts : parts + 5]
    out_ref, f_ref, v_ref = refs[-3:]
    rows, cols = out_ref.shape[2:]
    bands = rows // SUB + 2
    blank = jnp.zeros((SUB, cols), jnp.float32)
    for edge in (0, bands + 1):
        v_ref[edge * SUB : (edge + 1) * SUB] = blank
    for edge in (0, bands - 1):
        f_ref[edge * SUB : (edge + 1) * SUB] = blank
    f_ref[SUB - halo : SUB] = above_ref[0, 0]
    f_ref[SUB + rows : SUB + rows + halo] = below_ref[0, 0]
    for band in range(rows // SUB):
        at = slice(band * SUB, (band + 1) * SUB)
        value = field_refs[0][0, 0, at]
        for ref in field_refs[1:]:
            value += ref[0, 0, at]
        f_ref[SUB + band * SUB : SUB + (band + 1) * SUB] = value - share * (
            sum_ref[0, at] + other_ref[0, at]
        )
    for step in range(NSTEP):
        for band in range(bands):
            at = slice(band * SUB, (band + 1) * SUB)
            v_ref[SUB + band * SUB : 2 * SUB + band * SUB] = rate_ref[at] * f_ref[at]
        last = step == NSTEP - 1
        for band in range(1, bands - 1) if last else range(bands):
            at = slice(band * SUB, (band + 1) * SUB)
            base = SUB + band * SUB
            v = v_ref[base : base + SUB]
            value = (
                f_ref[at]
                + v_ref[base + 1 : base + 1 + SUB]
                + v_ref[base - 1 : base - 1 + SUB]
                + pltpu.roll(v, 1, 1)
                + pltpu.roll(v, cols - 1, 1)
                - 4.0 * v
            )
            if last:
                out_ref[0, 0, (band - 1) * SUB : band * SUB] = value
            else:
                f_ref[at] = value


def filtered(fields, sums, halos, rate, start, total, ensemble, previous):
    members, size, rows, cols = fields[0].shape
    halo = halos[0].shape[2]
    plane = pl.BlockSpec((1, 1, rows, cols), lambda i, k: (k, i, 0, 0))
    shared = pl.BlockSpec((1, rows, cols), lambda i, k: (i, 0, 0))
    edge = pl.BlockSpec((1, 1, halo, cols), lambda i, k: (k, i, 0, 0))
    operands = [*fields, *sums, *halos, rate]
    in_specs = [plane] * len(fields) + [shared] * 2 + [edge] * 2
    in_specs.append(pl.BlockSpec(rate.shape, lambda i, k: (0, 0)))
    aliases = {}
    if previous is not None:
        aliases = {len(operands): 0}
        operands.append(previous)
        in_specs.append(pl.BlockSpec(memory_space=pl.ANY))
    return pl.pallas_call(
        functools.partial(filter_kernel, len(fields), halo, 1.0 / ensemble),
        grid=(size, members),
        in_specs=in_specs,
        out_specs=pl.BlockSpec((1, 1, rows, cols), lambda i, k: (i + start, k, 0, 0)),
        out_shape=jax.ShapeDtypeStruct((total, members, rows, cols), jnp.float32),
        scratch_shapes=[
            pltpu.VMEM((rows + 2 * SUB, cols), jnp.float32),
            pltpu.VMEM((rows + 4 * SUB, cols), jnp.float32),
        ],
        input_output_aliases=aliases,
        cost_estimate=pl.CostEstimate(
            flops=40 * NSTEP * size * members * rows * cols,
            bytes_accessed=16 * size * members * rows * cols,
            transcendentals=0,
        ),
        name="filter",
    )(*operands)


def edges_from_neighbours(top, bottom):
    size = lax.axis_size("state")
    up = [(i, i + 1) for i in range(size - 1)]
    down = [(j, i) for i, j in up]
    return lax.ppermute(bottom, "state", up), lax.ppermute(top, "state", down)


def halves_of_sum(value):
    size = lax.axis_size("member")
    reach = 1
    other = jnp.zeros_like(value)
    if size & (size - 1):
        value, other = lax.psum(value, "member"), other
        return value, other
    while reach < size:
        pairs = [(i, i ^ reach) for i in range(size)]
        value = value + other if reach > 1 else value
        other = lax.ppermute(value, "member", pairs)
        reach *= 2
    return value, other


def compute(members, slot_grad, diffusivity, vertical):
    ensemble = members.shape[1] * lax.axis_size("member")
    levels, rows = members.shape[2:4]
    groups = lax.axis_size("tm")
    own = levels // groups
    here = lax.axis_index("tm")
    chunks = level_chunks(own)
    halo = NSTEP
    scaled = vertical.T * float(ensemble - 1) ** (-0.5)
    eye = jnp.eye(SUB, dtype=jnp.float32)

    def weights(shift):
        first = lax.rem(here + shift, groups) * own
        chosen = lax.dynamic_slice_in_dim(scaled, first, own, 0)
        return (chosen[:, None, :, None] * eye[None, :, None, :]).reshape(own * SUB, levels * SUB)

    share = 1.0 / ensemble

    def member_sums(fields):
        local = functools.reduce(jnp.add, [f[k] for f in fields for k in range(f.shape[0])])
        return halves_of_sum(local)

    arrived = []
    for shift in range(1, groups):
        outgoing = mixed_levels(members, slot_grad, weights(shift), chunks)
        pairs = [(i, (i + shift) % groups) for i in range(groups)]
        parts = []
        for index, part in enumerate(outgoing):
            if index:
                total = member_sums([part])
                part = part - ((total[0] + total[1]) * share)[None]
            parts.append(lax.ppermute(part, "tm", pairs))
        arrived.append(parts)
    mine = mixed_levels(members, slot_grad, weights(0), chunks)

    above, below = edges_from_neighbours(diffusivity[:halo], diffusivity[rows - halo :])
    blank = jnp.zeros((SUB - halo, diffusivity.shape[1]), jnp.float32)
    rate = jnp.concatenate([blank, above, diffusivity, below, blank], axis=0)

    early = [member_sums([part]) for part in mine[1:]]
    first = [mine[0]] + [parts[0] for parts in arrived]
    centres = [member_sums(first), *early]

    result = None
    for index, (start, size) in enumerate(chunks):
        fields = [mine[index]] + [parts[index] for parts in arrived]
        sums = centres[index]

        def edge(at):
            value = functools.reduce(jnp.add, [f[:, :, at] for f in fields])
            return value - (sums[0][:, at] + sums[1][:, at])[None] * share

        halos = edges_from_neighbours(edge(slice(0, halo)), edge(slice(rows - halo, rows)))
        result = filtered(fields, sums, halos, rate, start, own, ensemble, result)
    return result


def solution(mesh):
    in_specs = (
        P("tm", "member", None, "state", None),
        P("tm", None, "state", None),
        P("state", None),
        P(),
    )
    out_specs = P("tm", "member", "state", None)
    return jax.shard_map(compute, mesh=mesh, in_specs=in_specs, out_specs=out_specs, check_vma=False)
```
